256 devices in a mesh: mem: 16 (over y, x), gx: 4 (over z_hi, core), gy: 4 (over z_lo).
Axes of the slice: x: 4, y: 4, z: 8 (z_hi: 2, z_lo: 4; z = z_hi * 4 + z_lo), core: 2. Of those that a mesh axis runs over, the one named last changes fastest.
Arguments:
- field: bfloat16 [16, 512, 512, 128], P('mem', 'gx', 'gy'), may hold values from -6 to 6
- spectral: bfloat16 [3, 32, 2, 32, 128, 128], P(None, ('gx', 'gy'), None, None, 'mem'), may hold values from -0.0546875 to 0.0546875
- pointwise: bfloat16 [3, 128, 128], replicated, may hold values from -0.5 to 0.5
- bias: float32 [3, 128], replicated, may hold values from -3 to 3
Outputs:
- field_out: bfloat16 [16, 512, 512, 128], P('mem', 'gx', 'gy')
The draws below stay inside these ranges and needn't reach their ends.
All inputs are finite; a program needn't handle non-finite values.
Results may differ from the reference program's by a relative error of at most 0.02.
Values may be sent and summed in bfloat16 or wider, within the bound.
No kernel may reach another device: no remote copies, remote signals or barrier semaphores. Data moves between devices by JAX's collectives and lax.ppermute only.
A program may use at most 128 MiB of HBM per device.

```python
import math
import jax
import jax.numpy as jnp
from jax import lax

C = 128
KX = 32
KY = 32
NX = 512
NY = 512
LAYERS = 3
MEMBERS = 16
CXD = 128
N_GX = 4


def level_of(key, extent, cuts, least, largest):
    loudness, own = 1.0, jax.random.fold_in(key, 6)
    for axis_at, blocks in cuts:
        draws = jnp.exp(jax.random.uniform(jax.random.fold_in(own, axis_at), (blocks,), jnp.float32, least / len(cuts), largest / len(cuts)))
        loudness = loudness * jnp.repeat(draws, extent[axis_at] // blocks).reshape([-1 if axis == axis_at else 1 for axis in range(len(extent))])
    return loudness


def centred(stream_key, extent, scale, most, pieces=(), kind=jnp.bfloat16):
    array = jax.random.normal(stream_key, extent, jnp.float32) * scale
    if len(pieces) > 0:
        array = level_of(stream_key, extent, pieces, -0.22, 0.18) * array
    return jnp.clip(array, min=-most, max=most).astype(kind)


def setup_inputs(seed: int = 0) -> dict:
    streams_of = jax.random.split(jax.random.key(seed), 5)
    field = centred(streams_of[0], (MEMBERS, NX, NY, C), 1.0, 6.0, ((0, 16), (1, 4), (2, 4)))
    spectral = centred(streams_of[1], (LAYERS, KX, 2, KY, C, C), (100 * C) ** -0.5, 0.0546875, ((1, 16), (4, 16)))
    pointwise = centred(streams_of[2], (LAYERS, C, C), C ** -0.5, 0.5)
    bias = centred(streams_of[3], (LAYERS, C), 0.5, 3.0, (), jnp.float32)
    return {"field": field, "spectral": spectral, "pointwise": pointwise, "bias": bias}


def phase_angles(frequency, position, period):
    product = frequency[:, None] * position[None, :] % period
    return 2.0 * math.pi / period * product.astype(jnp.float32)

def x_frequencies():
    index = jnp.arange(KX, dtype=jnp.int32)
    return jnp.where(index < KX // 2, index, NX - KX + index)

def mode_product(coeffs, weights):
    coeffs = coeffs.astype(jnp.float32)
    weights = weights.astype(jnp.float32)
    real_part = jnp.einsum('kqi,kqio->kqo', coeffs[:, 0], weights[:, 0]) - jnp.einsum('kqi,kqio->kqo', coeffs[:, 1], weights[:, 1])
    imag_part = jnp.einsum('kqi,kqio->kqo', coeffs[:, 0], weights[:, 1]) + jnp.einsum('kqi,kqio->kqo', coeffs[:, 1], weights[:, 0])
    return jnp.stack([real_part, imag_part], axis=1)

def reference(field, spectral, pointwise, bias):
    positions_x = jnp.arange(NX, dtype=jnp.int32)
    positions_y = jnp.arange(NY, dtype=jnp.int32)
    angles_x = phase_angles(x_frequencies(), positions_x, NX)
    cosine_x = jnp.cos(angles_x).astype(jnp.bfloat16)
    sine_x = jnp.sin(angles_x).astype(jnp.bfloat16)
    forward_x = jnp.concatenate([cosine_x, -sine_x], axis=0)
    inverse_x = forward_x.T
    banded_x = forward_x.reshape(2 * KX, N_GX, CXD).astype(jnp.float32)
    angles_y = phase_angles(jnp.arange(KY, dtype=jnp.int32), positions_y, NY)
    cosine_y = jnp.cos(angles_y).T.astype(jnp.bfloat16)
    sine_y = jnp.sin(angles_y).T.astype(jnp.bfloat16)
    forward_y = jnp.concatenate([jnp.concatenate([cosine_y, -sine_y], axis=1), jnp.concatenate([sine_y, cosine_y], axis=1)], axis=0)
    doubling = jnp.where(jnp.arange(KY) == 0, 1.0, 2.0).astype(jnp.float32)[:, None]
    wcos = doubling * jnp.cos(angles_y)
    wsin = doubling * jnp.sin(angles_y)
    inverse_y = jnp.concatenate([jnp.concatenate([wcos, wsin], axis=1), jnp.concatenate([-wsin, wcos], axis=1)], axis=0).astype(jnp.bfloat16)
    scale_fwd = 1.0 / math.sqrt(NX * NY)
    scale_inv = 1.0 / math.sqrt(2 * KX * KY)

    def member_step(state):
        for level in range(LAYERS):
            bands = state.reshape(N_GX, CXD, NY, C).astype(jnp.float32)
            partial_x = jnp.einsum('kbx,bxyc->bkyc', banded_x, bands).astype(jnp.bfloat16)
            joined = jnp.concatenate([partial_x[:, :KX], partial_x[:, KX:]], axis=2)
            modes = jnp.einsum('bkyc,yq->kqc', joined.astype(jnp.float32), forward_y.astype(jnp.float32)) * scale_fwd
            modes = modes.reshape(KX, 2, KY, C).astype(jnp.bfloat16)
            mixed_modes = mode_product(modes, spectral[level]).astype(jnp.bfloat16)
            qmix = jnp.einsum('kqc,qy->kyc', mixed_modes.reshape(KX, 2 * KY, C).astype(jnp.float32), inverse_y.astype(jnp.float32)).astype(jnp.bfloat16)
            stacked = jnp.concatenate([qmix[:, :NY], qmix[:, NY:]], axis=0)
            spatial = jnp.einsum('xk,kyc->xyc', inverse_x.astype(jnp.float32), stacked.astype(jnp.float32))
            linear = jnp.dot(state.reshape(NX * NY, C), pointwise[level], preferred_element_type=jnp.float32).reshape(NX, NY, C)
            mixed = spatial * scale_inv + linear + bias[level].astype(jnp.float32)
            state = jax.nn.gelu(mixed, approximate=False).astype(jnp.bfloat16)
        return state
    return lax.map(member_step, field)
```

```python
import math

import jax
import jax.numpy as jnp
from jax import lax
from jax.experimental import pallas as pl
from jax.experimental.pallas import tpu as pltpu
from jax.sharding import PartitionSpec as P


KX = 32
KY = 32
NX = 512
NY = 512
LAYERS = 3
GRID = ("gx", "gy")
ZN = 8
RC = 4 * KY
SC = RC + 4
SG = 2 * KY + 4


def grid_index(z, core):
    return ((z // 4) * 2 + core) * 4 + z % 4


PAIR = [(grid_index(z, c), grid_index(z, 1 - c)) for z in range(ZN) for c in range(2)]
LINES = [[grid_index(z, c) for z in range(ZN)] for c in range(2)]


def angle_tables(rows_here, cols_here):
    gx = lax.axis_index("gx")
    gy = lax.axis_index("gy")
    row = lax.broadcasted_iota(jnp.int32, (KX + KY, 128), 0)
    lane = lax.broadcasted_iota(jnp.int32, (KX + KY, 128), 1)
    z = row % ZN
    core = (gx + (row // ZN) % 2) % 2
    index_x = 2 * (((z // 4) * 2 + core) * 4 + z % 4) + row // (2 * ZN)
    freq_x = jnp.where(index_x < KX // 2, index_x, NX - KX + index_x)
    in_x = row < KX
    freq = jnp.where(in_x, freq_x, row - KX)
    position = lane + jnp.where(in_x, gx * rows_here, gy * cols_here)
    angles = 2.0 * math.pi / NX * (freq * position % NX).astype(jnp.float32)
    return jnp.cos(angles), jnp.sin(angles)


def dot(a, b):
    return jnp.dot(a, b, preferred_element_type=jnp.float32)


GROUP = 8
BLOCK = 16


def copies_in(hbm, buf, sems):
    return [
        pltpu.make_async_copy(hbm.at[pl.ds(n * BLOCK, BLOCK)], buf.at[pl.ds(n * BLOCK, BLOCK)], sems.at[n])
        for n in range(buf.shape[0] // BLOCK)
    ]


def forward_group(i, u_ref, fy, h_ref):
    for e in range(GROUP // 2):
        x = i * GROUP + 2 * e
        h = dot(fy, jnp.concatenate([u_ref[x], u_ref[x + 1]], axis=1))
        h_ref[pl.ds(x, 2 * KY, stride=SC), :] = h[:, :128]
        h_ref[pl.ds(x + 1, 2 * KY, stride=SC), :] = h[:, 128:]


def modes_of(h_ref, m_ref, fx_ref, keep_ref, send_ref):
    fx = fx_ref[...]
    for q in range(0, KY, 2):
        rhs = jnp.concatenate(
            [
                jnp.concatenate(
                    [
                        h_ref[pl.ds((part * KY + q + d) * SC, 128), :].astype(jnp.bfloat16)
                        for part in range(2)
                    ],
                    axis=0,
                )
                for d in range(2)
            ],
            axis=1,
        )
        out = dot(fx, rhs)
        for d in range(2):
            for s in range(4):
                m_ref[pl.ds((q + d) * 4 + s, 16, stride=SC), :] = out[
                    16 * s : 16 * s + 16, 128 * d : 128 * d + 128
                ]
    for k in range(ZN):
        keep_ref[k] = m_ref[pl.ds(k * SC, RC), :]
        send_ref[k] = m_ref[pl.ds((ZN + k) * SC, RC), :].astype(jnp.bfloat16)


def first_kernel(
    u_hbm, cos_ref, sin_ref,
    keep_ref, send_ref, fx_ref, ix_ref, fy_ref, iy_ref,
    u_buf, h_ref, m_ref, sems,
):
    loads = copies_in(u_hbm, u_buf, sems)
    for c in loads:
        c.start()
    cx, cy = cos_ref[:KX], cos_ref[KX:]
    sx, sy = sin_ref[:KX], sin_ref[KX:]
    bf16 = jnp.bfloat16
    left = jnp.concatenate([cx, -sx], axis=0)
    right = jnp.concatenate([sx, cx], axis=0)
    table = jnp.concatenate([left, right], axis=1).astype(bf16)
    fx_ref[...] = (table.astype(jnp.float32) * (1.0 / math.sqrt(NX * NY))).astype(bf16)
    blank = jnp.zeros((128 - 2 * KX, 128), jnp.float32)
    ix_ref[:128] = jnp.concatenate([left, blank], axis=0).T[:, : 2 * KX].astype(bf16)
    ix_ref[128:] = jnp.concatenate([right, blank], axis=0).T[:, : 2 * KX].astype(bf16)
    fy_ref[...] = jnp.concatenate([cy, -sy], axis=0).astype(bf16)
    double = jnp.where(lax.broadcasted_iota(jnp.int32, (KY, 128), 0) == 0, 1.0, 2.0)
    iy_ref[...] = jnp.concatenate([double * cy, -(double * sy), blank], axis=0).T.astype(bf16)
    per = BLOCK // GROUP

    for n, c in enumerate(loads):
        c.wait()

        def step(i, carry):
            forward_group(i, u_buf, fy_ref[...], h_ref)
            return carry

        lax.fori_loop(n * per, (n + 1) * per, step, 0)
    modes_of(h_ref, m_ref, fx_ref, keep_ref, send_ref)


def layer_body(u_hbm, own_ref, oth_ref, ix_ref, iy_ref, w_ref, b_ref, out_hbm, u_buf, bs_ref, g_ref, sems, forward):
    loads = copies_in(u_hbm, u_buf, sems.at[0])
    for c in loads:
        c.start()
    for k in range(ZN):
        bs_ref[pl.ds(k * SC, RC), :] = own_ref[k].astype(jnp.float32)
        bs_ref[pl.ds((ZN + k) * SC, RC), :] = oth_ref[k].astype(jnp.float32)
    scale = 1.0 / math.sqrt(2 * KX * KY)
    ix = ix_ref[...]
    for q in range(0, KY, 2):
        rhs = jnp.concatenate(
            [
                jnp.concatenate(
                    [bs_ref[pl.ds((q + d) * 4 + s, 16, stride=SC), :] for s in range(4)], axis=0
                ).astype(jnp.bfloat16)
                for d in range(2)
            ],
            axis=1,
        )
        for part in range(2):
            g = dot(ix[128 * part : 128 * part + 128], rhs) * scale
            for d in range(2):
                g_ref[pl.ds(part * KY + q + d, 128, stride=SG), :] = g[:, 128 * d : 128 * d + 128]
    for c in loads:
        c.wait()
    steps = u_buf.shape[0] // GROUP

    def store(i):
        return pltpu.make_async_copy(
            u_buf.at[pl.ds(i * GROUP, GROUP)], out_hbm.at[pl.ds(i * GROUP, GROUP)], sems.at[1, i]
        )

    def point(i):
        w = w_ref[...]
        iy = iy_ref[...]
        bias = b_ref[...]
        pad = jnp.zeros((128 - 2 * KY, 128), jnp.bfloat16)
        for e in range(GROUP):
            x = i * GROUP + e
            gx = g_ref[pl.ds(x * SG, 2 * KY), :].astype(jnp.bfloat16)
            lhs = jnp.concatenate([u_buf[x], iy], axis=1)
            rhs = jnp.concatenate([w, gx, pad], axis=0)
            z = dot(lhs, rhs) + bias
            half = 0.5 * z
            u_buf[x] = (half + half * lax.erf(z * math.sqrt(0.5))).astype(jnp.bfloat16)

    def step(i, carry):
        if forward is not None:
            forward(i - 1)
        point(i)
        store(i).start()
        return carry

    point(0)
    store(0).start()
    lax.fori_loop(1, steps, step, 0)
    if forward is not None:
        forward(steps - 1)

    def finish():
        for i in range(steps):
            store(i).wait()

    return finish


def mid_kernel(
    u_hbm, own_ref, oth_ref, ix_ref, iy_ref, w_ref, b_ref, fy_ref, fx_ref,
    out_hbm, keep_ref, send_ref, u_buf, bs_ref, g_ref, h_ref, m_ref, sems,
):
    def forward(i):
        forward_group(i, u_buf, fy_ref[...], h_ref)

    finish = layer_body(
        u_hbm, own_ref, oth_ref, ix_ref, iy_ref, w_ref, b_ref, out_hbm, u_buf, bs_ref, g_ref, sems, forward
    )
    modes_of(h_ref, m_ref, fx_ref, keep_ref, send_ref)
    finish()


def last_kernel(
    u_hbm, own_ref, oth_ref, ix_ref, iy_ref, w_ref, b_ref, out_hbm, u_buf, bs_ref, g_ref, sems
):
    layer_body(
        u_hbm, own_ref, oth_ref, ix_ref, iy_ref, w_ref, b_ref, out_hbm, u_buf, bs_ref, g_ref, sems, None
    )()


def few_kernel(a_ref, w_ref, out_ref, as_ref, bs_ref):
    members = a_ref.shape[0]
    as_ref[...] = a_ref[...].astype(jnp.float32).reshape(members * 8, 128)
    for e in range(2):
        for jj in range(2):
            w = jnp.concatenate(
                [
                    w_ref[:, jj, ri, e].astype(jnp.float32).reshape(128, 128).astype(jnp.bfloat16)
                    for ri in range(2)
                ],
                axis=1,
            )
            row_re = e * 4 + jj
            row_im = e * 4 + 2 + jj
            re = dot(as_ref[pl.ds(row_re, members, stride=8), :].astype(jnp.bfloat16), w)
            im = dot(as_ref[pl.ds(row_im, members, stride=8), :].astype(jnp.bfloat16), w)
            bs_ref[pl.ds(row_re, members, stride=8), :] = re[:, :128] - im[:, 128:]
            bs_ref[pl.ds(row_im, members, stride=8), :] = re[:, 128:] + im[:, :128]
    out_ref[...] = bs_ref[...].reshape(members, 8, 128).astype(jnp.bfloat16)


def many_kernel(s_ref, w_hbm, out_ref, w_buf, sems):
    loads = [
        pltpu.make_async_copy(w_hbm.at[:, :, pl.ds(4 * b, 4)], w_buf.at[b], sems.at[b])
        for b in range(KY // 4)
    ]
    for c in loads:
        c.start()
    a = s_ref[0].astype(jnp.float32)
    for k in range(1, ZN):
        a = a + s_ref[k].astype(jnp.float32)
    row = lax.broadcasted_iota(jnp.int32, (16, 128), 0)
    lower = row % 4 < 2
    blocks = []
    for b in range(KY // 4):
        rows = a[16 * b : 16 * b + 16]
        acc = None
        loads[b].wait()
        for dq in range(4):
            for jj in range(2):
                mine = (row == dq * 4 + jj) | (row == dq * 4 + 2 + jj)
                lhs = jnp.where(mine, rows, 0.0).astype(jnp.bfloat16)
                w = jnp.concatenate([w_buf[b, jj, 0, dq], w_buf[b, jj, 1, dq]], axis=1)
                part = dot(lhs, w)
                acc = part if acc is None else acc + part
        straight = acc[:, :128]
        cross = acc[:, 128:]
        up = jnp.concatenate([cross[2:], cross[:2]], axis=0)
        down = jnp.concatenate([cross[14:], cross[:14]], axis=0)
        blocks.append(jnp.where(lower, straight - up, straight + down).astype(jnp.bfloat16))
    full = jnp.concatenate(blocks, axis=0)
    for k in range(ZN):
        out_ref[k] = full


V = pl.BlockSpec(memory_space=pltpu.VMEM)
H = pl.BlockSpec(memory_space=pltpu.HBM)


def call(kernel, args, outs, scratch=(), in_hbm=(), out_hbm=(), alias=None, limit=24):
    args = [
        pltpu.with_memory_space_constraint(a, pltpu.HBM) if i in in_hbm else a for i, a in enumerate(args)
    ]
    outs = [pltpu.HBM(o.shape, o.dtype) if i in out_hbm else o for i, o in enumerate(outs)]
    return pl.pallas_call(
        kernel,
        out_shape=outs,
        in_specs=[H if i in in_hbm else V for i in range(len(args))],
        out_specs=[H if i in out_hbm else V for i in range(len(outs))],
        scratch_shapes=list(scratch),
        input_output_aliases=alias or {},
        compiler_params=pltpu.CompilerParams(vmem_limit_bytes=limit << 20),
    )(*args)


def local(field, spectral, pointwise, bias):
    u = field[0]
    rows_here, cols_here, channels = u.shape
    members = lax.axis_size("mem")
    bf16, f32 = jnp.bfloat16, jnp.float32
    sds = jax.ShapeDtypeStruct
    dma = pltpu.SemaphoreType.DMA
    chunks = [sds((ZN, RC, channels), f32), sds((ZN, RC, channels), bf16)]
    ub = pltpu.VMEM(u.shape, bf16)
    bs = pltpu.VMEM((2 * ZN * SC, channels), f32)
    gs = pltpu.VMEM((rows_here * SG, channels), f32)
    hs = pltpu.VMEM((2 * KY * SC, channels), f32)
    blocks, steps = rows_here // BLOCK, rows_here // GROUP

    weights = {
        level: lax.all_gather(spectral[level], "mem", axis=3, tiled=True) for level in range(1, LAYERS)
    }
    first = spectral[0].reshape(2, 2, members, 2, 8, channels)
    first = jnp.moveaxis(first, 2, 0)
    first = lax.all_to_all(first, "mem", 0, 0, tiled=True)

    cosines, sines = angle_tables(rows_here, cols_here)
    keep, send, forward_x, inverse_x, forward_y, inverse_y = call(
        first_kernel,
        (u, cosines, sines),
        [
            *chunks,
            sds((2 * KX, 2 * rows_here), bf16),
            sds((2 * rows_here, 2 * KX), bf16),
            sds((2 * KY, cols_here), bf16),
            sds((cols_here, 128), bf16),
        ],
        (ub, hs, bs, dma((blocks,))),
        in_hbm=(0,),
    )
    for level in range(LAYERS):
        other = lax.ppermute(send, GRID, PAIR)
        paired = (keep + other.astype(f32)).astype(bf16)
        if level == 0:
            paired, first = lax.optimization_barrier((paired, first))
        parts = lax.all_to_all(paired, GRID, 0, 0, axis_index_groups=LINES, tiled=True)
        if level == 0:
            coeffs = parts.astype(f32).sum(axis=0).astype(bf16).reshape(members, 8, channels)
            coeffs = lax.all_to_all(coeffs, "mem", 0, 0, tiled=True)
            small = pltpu.VMEM((members * 8, channels), f32)
            (mixed,) = call(few_kernel, (coeffs, first), [sds((members, 8, channels), bf16)], (small, small))
            mixed = lax.all_to_all(mixed, "mem", 0, 0, tiled=True).reshape(RC, channels)
            mixed = jnp.broadcast_to(mixed, (ZN, RC, channels))
        else:
            (mixed,) = call(
                many_kernel,
                (parts, weights[level]),
                [sds((ZN, RC, channels), bf16)],
                (pltpu.VMEM((KY // 4, 2, 2, 4, channels, channels), bf16), dma((KY // 4,))),
                in_hbm=(1,),
            )
        own = lax.all_to_all(mixed, GRID, 0, 0, axis_index_groups=LINES, tiled=True)
        oth = lax.ppermute(own, GRID, PAIR)
        args = (u, own, oth, inverse_x, inverse_y, pointwise[level], bias[level][None])
        if level < LAYERS - 1:
            u, keep, send = call(
                mid_kernel,
                (*args, forward_y, forward_x),
                [sds(u.shape, bf16), *chunks],
                (ub, bs, gs, hs, bs, dma((2, steps))),
                in_hbm=(0,),
                out_hbm=(0,),
            )
        else:
            (u,) = call(
                last_kernel, args, [sds(u.shape, bf16)], (ub, bs, gs, dma((2, steps))),
                in_hbm=(0,), out_hbm=(0,),
            )
    return u[None]


def solution(mesh):
    in_specs = (
        P("mem", "gx", "gy", None),
        P(None, ("gx", "gy"), None, None, "mem", None),
        P(),
        P(),
    )
    out_specs = P("mem", "gx", "gy", None)
    return jax.shard_map(local, mesh=mesh, in_specs=in_specs, out_specs=out_specs, check_vma=False)
```

```python
import math

import jax
import jax.numpy as jnp
from jax import lax
from jax.experimental import pallas as pl
from jax.experimental.pallas import tpu as pltpu
from jax.sharding import PartitionSpec as P


KX = 32
KY = 32
NX = 512
NY = 512
LAYERS = 3
GRID = ("gx", "gy")
ZN = 8
RC = 4 * KY
SC = RC + 4
SG = 2 * KY + 4

SIDE = 4
SLICE = 32


def shift(dy, dx):
    return [
        (y * SIDE + x, (y + dy) % SIDE * SIDE + (x + dx) % SIDE) for y in range(SIDE) for x in range(SIDE)
    ]


def grid_index(z, core):
    return ((z // 4) * 2 + core) * 4 + z % 4


PAIR = [(grid_index(z, c), grid_index(z, 1 - c)) for z in range(ZN) for c in range(2)]
LINES = [[grid_index(z, c) for z in range(ZN)] for c in range(2)]


def angle_tables(rows_here, cols_here):
    gx = lax.axis_index("gx")
    gy = lax.axis_index("gy")
    row = lax.broadcasted_iota(jnp.int32, (KX + KY, 128), 0)
    lane = lax.broadcasted_iota(jnp.int32, (KX + KY, 128), 1)
    z = row % ZN
    core = (gx + (row // ZN) % 2) % 2
    index_x = 2 * (((z // 4) * 2 + core) * 4 + z % 4) + row // (2 * ZN)
    freq_x = jnp.where(index_x < KX // 2, index_x, NX - KX + index_x)
    in_x = row < KX
    freq = jnp.where(in_x, freq_x, row - KX)
    position = lane + jnp.where(in_x, gx * rows_here, gy * cols_here)
    angles = 2.0 * math.pi / NX * (freq * position % NX).astype(jnp.float32)
    return jnp.cos(angles), jnp.sin(angles)


def dot(a, b):
    return jnp.dot(a, b, preferred_element_type=jnp.float32)


GROUP = 16


def copy_in(hbm, buf, sems, i):
    rows = pl.ds(i * GROUP, GROUP)
    return pltpu.make_async_copy(hbm.at[rows], buf.at[rows], sems.at[i])


def forward_group(i, u_ref, fy, h_ref):
    for e in range(GROUP // 2):
        x = i * GROUP + 2 * e
        h = dot(fy, jnp.concatenate([u_ref[x], u_ref[x + 1]], axis=1))
        h_ref[pl.ds(x, 2 * KY, stride=SC), :] = h[:, :128]
        h_ref[pl.ds(x + 1, 2 * KY, stride=SC), :] = h[:, 128:]


def modes_of(h_ref, m_ref, fx_ref, keep_ref, send_ref):
    fx = fx_ref[...]
    for q in range(0, KY, 2):
        rhs = jnp.concatenate(
            [
                jnp.concatenate(
                    [
                        h_ref[pl.ds((part * KY + q + d) * SC, 128), :].astype(jnp.bfloat16)
                        for part in range(2)
                    ],
                    axis=0,
                )
                for d in range(2)
            ],
            axis=1,
        )
        out = dot(fx, rhs)
        for d in range(2):
            for s in range(4):
                m_ref[pl.ds((q + d) * 4 + s, 16, stride=SC), :] = out[
                    16 * s : 16 * s + 16, 128 * d : 128 * d + 128
                ]
    for k in range(ZN):
        keep_ref[k] = m_ref[pl.ds(k * SC, RC), :]
        send_ref[k] = m_ref[pl.ds((ZN + k) * SC, RC), :].astype(jnp.bfloat16)


def first_kernel(
    u_hbm, cos_ref, sin_ref,
    keep_ref, send_ref, fx_ref, ix_ref, fy_ref, iy_ref,
    u_buf, h_ref, m_ref, sems,
):
    steps = u_buf.shape[0] // GROUP
    for i in range(steps):
        copy_in(u_hbm, u_buf, sems, i).start()
    cx, cy = cos_ref[:KX], cos_ref[KX:]
    sx, sy = sin_ref[:KX], sin_ref[KX:]
    bf16 = jnp.bfloat16
    left = jnp.concatenate([cx, -sx], axis=0)
    right = jnp.concatenate([sx, cx], axis=0)
    table = jnp.concatenate([left, right], axis=1).astype(bf16)
    fx_ref[...] = (table.astype(jnp.float32) * (1.0 / math.sqrt(NX * NY))).astype(bf16)
    blank = jnp.zeros((128 - 2 * KX, 128), jnp.float32)
    ix_ref[:128] = jnp.concatenate([left, blank], axis=0).T[:, : 2 * KX].astype(bf16)
    ix_ref[128:] = jnp.concatenate([right, blank], axis=0).T[:, : 2 * KX].astype(bf16)
    fy_ref[...] = jnp.concatenate([cy, -sy], axis=0).astype(bf16)
    double = jnp.where(lax.broadcasted_iota(jnp.int32, (KY, 128), 0) == 0, 1.0, 2.0)
    iy_ref[...] = jnp.concatenate([double * cy, -(double * sy), blank], axis=0).T.astype(bf16)

    def step(i, carry):
        copy_in(u_hbm, u_buf, sems, i).wait()
        forward_group(i, u_buf, fy_ref[...], h_ref)
        return carry

    lax.fori_loop(0, steps, step, 0)
    modes_of(h_ref, m_ref, fx_ref, keep_ref, send_ref)


def layer_body(u_hbm, own_ref, oth_ref, ix_ref, iy_ref, w_ref, b_ref, out_hbm, u_buf, bs_ref, g_ref, sems, forward):
    steps = u_buf.shape[0] // GROUP
    for i in range(steps):
        copy_in(u_hbm, u_buf, sems.at[0], i).start()

    def unpack(k, carry):
        bs_ref[pl.ds(k * SC, RC), :] = own_ref[k].astype(jnp.float32)
        bs_ref[pl.ds((ZN + k) * SC, RC), :] = oth_ref[k].astype(jnp.float32)
        return carry

    lax.fori_loop(0, ZN, unpack, 0)
    scale = 1.0 / math.sqrt(2 * KX * KY)
    ix = ix_ref[...]
    for q in range(0, KY, 2):
        rhs = jnp.concatenate(
            [
                jnp.concatenate(
                    [bs_ref[pl.ds((q + d) * 4 + s, 16, stride=SC), :] for s in range(4)], axis=0
                ).astype(jnp.bfloat16)
                for d in range(2)
            ],
            axis=1,
        )
        for part in range(2):
            g = dot(ix[128 * part : 128 * part + 128], rhs) * scale
            for d in range(2):
                g_ref[pl.ds(part * KY + q + d, 128, stride=SG), :] = g[:, 128 * d : 128 * d + 128]

    def store(i):
        return pltpu.make_async_copy(
            u_buf.at[pl.ds(i * GROUP, GROUP)], out_hbm.at[pl.ds(i * GROUP, GROUP)], sems.at[1, i]
        )

    def point(i):
        w = w_ref[...]
        iy = iy_ref[...]
        bias = b_ref[...]
        pad = jnp.zeros((128 - 2 * KY, 128), jnp.bfloat16)
        for e in range(GROUP):
            x = i * GROUP + e
            gx = g_ref[pl.ds(x * SG, 2 * KY), :].astype(jnp.bfloat16)
            lhs = jnp.concatenate([u_buf[x], iy], axis=1)
            rhs = jnp.concatenate([w, gx, pad], axis=0)
            z = dot(lhs, rhs) + bias
            half = 0.5 * z
            u_buf[x] = (half + half * lax.erf(z * math.sqrt(0.5))).astype(jnp.bfloat16)

    def step(i, carry):
        copy_in(u_hbm, u_buf, sems.at[0], i).wait()
        if forward is not None:
            forward(i - 1)
        point(i)
        store(i).start()
        return carry

    copy_in(u_hbm, u_buf, sems.at[0], 0).wait()
    point(0)
    store(0).start()
    lax.fori_loop(1, steps, step, 0)
    if forward is not None:
        forward(steps - 1)

    def finish():
        for i in range(steps):
            store(i).wait()

    return finish


def mid_kernel(
    u_hbm, own_ref, oth_ref, ix_ref, iy_ref, w_ref, b_ref, fy_ref, fx_ref,
    out_hbm, keep_ref, send_ref, u_buf, bs_ref, g_ref, h_ref, m_ref, sems,
):
    def forward(i):
        forward_group(i, u_buf, fy_ref[...], h_ref)

    finish = layer_body(
        u_hbm, own_ref, oth_ref, ix_ref, iy_ref, w_ref, b_ref, out_hbm, u_buf, bs_ref, g_ref, sems, forward
    )
    modes_of(h_ref, m_ref, fx_ref, keep_ref, send_ref)
    finish()


def last_kernel(
    u_hbm, own_ref, oth_ref, ix_ref, iy_ref, w_ref, b_ref, out_hbm, u_buf, bs_ref, g_ref, sems
):
    layer_body(
        u_hbm, own_ref, oth_ref, ix_ref, iy_ref, w_ref, b_ref, out_hbm, u_buf, bs_ref, g_ref, sems, None
    )()


def split_kernel(spectral_hbm, first_ref, *refs):
    outs, buf, sems = refs[:-2], refs[-2], refs[-1]
    first = pltpu.make_async_copy(spectral_hbm.at[0], first_ref, sems.at[0, 0])
    loads = [pltpu.make_async_copy(spectral_hbm.at[n + 1], buf.at[n], sems.at[0, n + 1]) for n in range(len(outs))]
    stores = [pltpu.make_async_copy(buf.at[n], out, sems.at[1, n + 1]) for n, out in enumerate(outs)]
    for c in loads:
        c.start()
    first.start()
    for load, store in zip(loads, stores):
        load.wait()
        store.start()
    first.wait()
    for c in stores:
        c.wait()


def turn_kernel(s_ref, *refs):
    outs, t_ref = refs[:-1], refs[-1]
    a = s_ref[0].astype(jnp.float32)
    for k in range(1, ZN):
        a = a + s_ref[k].astype(jnp.float32)
    t_ref[...] = a.T
    y = lax.axis_index("mem") // SIDE
    for k in range(SIDE):
        start = pl.multiple_of((y + k) % SIDE * SLICE, SLICE)
        outs[k][...] = t_ref[pl.ds(start, SLICE), :].astype(jnp.bfloat16)


def share_kernel(*refs):
    a_refs, w_refs, outs = refs[:SIDE], refs[SIDE : 2 * SIDE], refs[2 * SIDE : 3 * SIDE]
    t_ref, m_ref, w_buf, sems = refs[3 * SIDE :]
    x = lax.axis_index("mem") % SIDE
    loads = [
        pltpu.make_async_copy(w_refs[k], w_buf.at[(x + SIDE - k) % SIDE], sems.at[k]) for k in range(SIDE)
    ]
    for c in loads:
        c.start()
    t_ref[...] = jnp.concatenate([r[...].astype(jnp.float32) for r in a_refs], axis=0).T
    row = lax.broadcasted_iota(jnp.int32, (8, 128), 0)
    lane = lax.broadcasted_iota(jnp.int32, (8, 128), 1)
    own = lane // SLICE == row
    for c in loads:
        c.wait()
    for q in range(KY):
        for jj in range(2):
            at = [q * 4 + 2 * ri + jj for ri in range(2)]
            lhs = jnp.concatenate(
                [jnp.where(own, t_ref[r : r + 1, :], 0.0) for r in at], axis=0
            ).astype(jnp.bfloat16)
            w = jnp.concatenate(
                [
                    jnp.concatenate([w_buf[x, jj, ri, q].astype(jnp.float32) for x in range(SIDE)] * SIDE, axis=0)
                    for ri in range(2)
                ],
                axis=1,
            ).astype(jnp.bfloat16)
            out = dot(lhs, w)
            re, im = out[:8], out[8:]
            m_ref[pl.ds(at[0], 8, stride=SC), :] = re[:, :128] - im[:, 128:]
            m_ref[pl.ds(at[1], 8, stride=SC), :] = re[:, 128:] + im[:, :128]
    for k in range(SIDE):
        outs[k][...] = m_ref[pl.ds(k * SC, RC), :].astype(jnp.bfloat16)


def total_kernel(*refs):
    out_ref = refs[-1]
    b = refs[0][...].astype(jnp.float32)
    for r in refs[1:-1]:
        b = b + r[...].astype(jnp.float32)
    b = b.astype(jnp.bfloat16)
    for k in range(ZN):
        out_ref[k] = b


def many_kernel(a_ref, w_hbm, out_ref, w_buf, sems):
    loads = [
        pltpu.make_async_copy(w_hbm.at[:, :, pl.ds(4 * b, 4)], w_buf.at[b], sems.at[b])
        for b in range(KY // 4)
    ]
    for c in loads:
        c.start()
    row = lax.broadcasted_iota(jnp.int32, (16, 128), 0)
    lower = row % 4 < 2
    blocks = []
    for b in range(KY // 4):
        rows = a_ref[16 * b : 16 * b + 16]
        acc = None
        loads[b].wait()
        for dq in range(4):
            for jj in range(2):
                mine = (row == dq * 4 + jj) | (row == dq * 4 + 2 + jj)
                lhs = jnp.where(mine, rows, 0)
                w = jnp.concatenate([w_buf[b, jj, 0, dq], w_buf[b, jj, 1, dq]], axis=1)
                part = dot(lhs, w)
                acc = part if acc is None else acc + part
        straight = acc[:, :128]
        cross = acc[:, 128:]
        up = jnp.concatenate([cross[2:], cross[:2]], axis=0)
        down = jnp.concatenate([cross[14:], cross[:14]], axis=0)
        blocks.append(jnp.where(lower, straight - up, straight + down).astype(jnp.bfloat16))
    full = jnp.concatenate(blocks, axis=0)
    for k in range(ZN):
        out_ref[k] = full


V = pl.BlockSpec(memory_space=pltpu.VMEM)
H = pl.BlockSpec(memory_space=pltpu.HBM)
A = pl.BlockSpec(memory_space=pl.ANY)


def call(kernel, args, outs, scratch=(), in_hbm=(), out_hbm=(), anywhere=(), limit=24):
    args = [
        pltpu.with_memory_space_constraint(a, pltpu.HBM) if i in in_hbm else a for i, a in enumerate(args)
    ]
    outs = [pltpu.HBM(o.shape, o.dtype) if i in out_hbm else o for i, o in enumerate(outs)]
    return pl.pallas_call(
        kernel,
        out_shape=outs,
        in_specs=[H if i in in_hbm else A if i in anywhere else V for i in range(len(args))],
        out_specs=[H if i in out_hbm else V for i in range(len(outs))],
        scratch_shapes=list(scratch),
        compiler_params=pltpu.CompilerParams(vmem_limit_bytes=limit << 20),
    )(*args)


def local(field, spectral, pointwise, bias):
    u = field[0]
    rows_here, cols_here, channels = u.shape
    bf16, f32 = jnp.bfloat16, jnp.float32
    sds = jax.ShapeDtypeStruct
    dma = pltpu.SemaphoreType.DMA
    chunks = [sds((ZN, RC, channels), f32), sds((ZN, RC, channels), bf16)]
    ub = pltpu.VMEM(u.shape, bf16)
    bs = pltpu.VMEM((2 * ZN * SC, channels), f32)
    gs = pltpu.VMEM((rows_here * SG, channels), f32)
    hs = pltpu.VMEM((2 * KY * SC, channels), f32)
    steps = rows_here // GROUP

    level_weights = sds(spectral.shape[1:], bf16)
    split = call(
        split_kernel, (spectral,), [level_weights] * LAYERS,
        (pltpu.VMEM((LAYERS - 1, *spectral.shape[1:]), bf16), dma((2, LAYERS))),
        in_hbm=(0,), out_hbm=tuple(range(1, LAYERS)),
    )
    weights = {}
    for level in range(1, LAYERS):
        weights[level] = lax.all_gather(split[level], "mem", axis=3, tiled=True)
    near = [split[0]]
    for k in range(1, SIDE):
        near.append(lax.ppermute(split[0], "mem", shift(0, k)))

    cosines, sines = angle_tables(rows_here, cols_here)
    keep, send, forward_x, inverse_x, forward_y, inverse_y = call(
        first_kernel,
        (u, cosines, sines),
        [
            *chunks,
            sds((2 * KX, 2 * rows_here), bf16),
            sds((2 * rows_here, 2 * KX), bf16),
            sds((2 * KY, cols_here), bf16),
            sds((cols_here, 128), bf16),
        ],
        (ub, hs, bs, dma((steps,))),
        in_hbm=(0,),
    )
    for level in range(LAYERS):
        other = lax.ppermute(send, GRID, PAIR)
        paired = (keep + other.astype(f32)).astype(bf16)
        parts = lax.all_to_all(paired, GRID, 0, 0, axis_index_groups=LINES, tiled=True)
        if level == 0:
            square = pltpu.VMEM((RC, channels), f32)
            slices = call(turn_kernel, (parts,), [sds((SLICE, RC), bf16)] * SIDE, (square,))
            slices = [slices[0]] + [lax.ppermute(slices[k], "mem", shift(k, 0)) for k in range(1, SIDE)]
            shares = call(
                share_kernel,
                (*slices, *near),
                [sds((RC, channels), bf16)] * SIDE,
                (
                    square,
                    pltpu.VMEM((8 * SC, channels), f32),
                    pltpu.VMEM((SIDE, *spectral.shape[1:]), bf16),
                    dma((SIDE,)),
                ),
                anywhere=tuple(range(SIDE, 2 * SIDE)),
            )
            shares = [shares[0]] + [lax.ppermute(shares[k], "mem", shift(-k, 0)) for k in range(1, SIDE)]
            (mixed,) = call(total_kernel, shares, [sds((ZN, RC, channels), bf16)])
        else:
            coeffs = parts.astype(f32).sum(axis=0).astype(bf16)
            (mixed,) = call(
                many_kernel,
                (coeffs, weights[level]),
                [sds((ZN, RC, channels), bf16)],
                (pltpu.VMEM((KY // 4, 2, 2, 4, channels, channels), bf16), dma((KY // 4,))),
                in_hbm=(1,),
            )
        own = lax.all_to_all(mixed, GRID, 0, 0, axis_index_groups=LINES, tiled=True)
        oth = lax.ppermute(own, GRID, PAIR)
        args = (u, own, oth, inverse_x, inverse_y, pointwise[level], bias[level][None])
        if level < LAYERS - 1:
            u, keep, send = call(
                mid_kernel,
                (*args, forward_y, forward_x),
                [sds(u.shape, bf16), *chunks],
                (ub, bs, gs, hs, bs, dma((2, steps))),
                in_hbm=(0,),
                out_hbm=(0,),
            )
        else:
            (u,) = call(
                last_kernel, args, [sds(u.shape, bf16)], (ub, bs, gs, dma((2, steps))),
                in_hbm=(0,), out_hbm=(0,),
            )
    return u[None]


def solution(mesh):
    in_specs = (
        P("mem", "gx", "gy", None),
        P(None, ("gx", "gy"), None, None, "mem", None),
        P(),
        P(),
    )
    out_specs = P("mem", "gx", "gy", None)
    return jax.shard_map(local, mesh=mesh, in_specs=in_specs, out_specs=out_specs, check_vma=False)
```

```python
import math

import jax
import jax.numpy as jnp
from jax import lax
from jax.experimental import pallas as pl
from jax.experimental.pallas import tpu as pltpu
from jax.sharding import PartitionSpec as P


KX = 32
KY = 32
NX = 512
NY = 512
LAYERS = 3
GRID = ("gx", "gy")
ZN = 8
RC = 4 * KY
SC = RC + 4
SG = 2 * KY + 4

SIDE = 4
SLICE = 32


def shift(dy, dx):
    return [
        (y * SIDE + x, (y + dy) % SIDE * SIDE + (x + dx) % SIDE) for y in range(SIDE) for x in range(SIDE)
    ]


def grid_index(z, core):
    return ((z // 4) * 2 + core) * 4 + z % 4


PAIR = [(grid_index(z, c), grid_index(z, 1 - c)) for z in range(ZN) for c in range(2)]
LINES = [[grid_index(z, c) for z in range(ZN)] for c in range(2)]


def angle_tables(rows_here, cols_here):
    gx = lax.axis_index("gx")
    gy = lax.axis_index("gy")
    row = lax.broadcasted_iota(jnp.int32, (KX + KY, 128), 0)
    lane = lax.broadcasted_iota(jnp.int32, (KX + KY, 128), 1)
    z = row % ZN
    core = (gx + (row // ZN) % 2) % 2
    index_x = 2 * (((z // 4) * 2 + core) * 4 + z % 4) + row // (2 * ZN)
    freq_x = jnp.where(index_x < KX // 2, index_x, NX - KX + index_x)
    in_x = row < KX
    freq = jnp.where(in_x, freq_x, row - KX)
    position = lane + jnp.where(in_x, gx * rows_here, gy * cols_here)
    angles = 2.0 * math.pi / NX * (freq * position % NX).astype(jnp.float32)
    return jnp.cos(angles), jnp.sin(angles)


def dot(a, b):
    return jnp.dot(a, b, preferred_element_type=jnp.float32)


GROUP = 32


def copy_in(hbm, buf, sems, i):
    rows = pl.ds(i * GROUP, GROUP)
    return pltpu.make_async_copy(hbm.at[rows], buf.at[rows], sems.at[i])


def forward_group(i, u_ref, fy, h_ref):
    for e in range(GROUP // 2):
        x = i * GROUP + 2 * e
        h = dot(fy, jnp.concatenate([u_ref[x], u_ref[x + 1]], axis=1))
        h_ref[pl.ds(x, 2 * KY, stride=SC), :] = h[:, :128]
        h_ref[pl.ds(x + 1, 2 * KY, stride=SC), :] = h[:, 128:]


def modes_of(h_ref, m_ref, fx_ref, keep_ref, send_ref):
    fx = fx_ref[...]
    for q in range(0, KY, 2):
        rhs = jnp.concatenate(
            [
                jnp.concatenate(
                    [
                        h_ref[pl.ds((part * KY + q + d) * SC, 128), :].astype(jnp.bfloat16)
                        for part in range(2)
                    ],
                    axis=0,
                )
                for d in range(2)
            ],
            axis=1,
        )
        out = dot(fx, rhs)
        for d in range(2):
            for s in range(4):
                m_ref[pl.ds((q + d) * 4 + s, 16, stride=SC), :] = out[
                    16 * s : 16 * s + 16, 128 * d : 128 * d + 128
                ]
    for k in range(ZN):
        keep_ref[k] = m_ref[pl.ds(k * SC, RC), :]
        send_ref[k] = m_ref[pl.ds((ZN + k) * SC, RC), :].astype(jnp.bfloat16)


def first_kernel(
    u_hbm, cos_ref, sin_ref,
    keep_ref, send_ref, fx_ref, ix_ref, fy_ref, iy_ref,
    u_buf, h_ref, m_ref, sems,
):
    steps = u_buf.shape[0] // GROUP
    for i in range(steps):
        copy_in(u_hbm, u_buf, sems, i).start()
    cx, cy = cos_ref[:KX], cos_ref[KX:]
    sx, sy = sin_ref[:KX], sin_ref[KX:]
    bf16 = jnp.bfloat16
    left = jnp.concatenate([cx, -sx], axis=0)
    right = jnp.concatenate([sx, cx], axis=0)
    table = jnp.concatenate([left, right], axis=1).astype(bf16)
    fx_ref[...] = (table.astype(jnp.float32) * (1.0 / math.sqrt(NX * NY))).astype(bf16)
    blank = jnp.zeros((128 - 2 * KX, 128), jnp.float32)
    ix_ref[:128] = jnp.concatenate([left, blank], axis=0).T[:, : 2 * KX].astype(bf16)
    ix_ref[128:] = jnp.concatenate([right, blank], axis=0).T[:, : 2 * KX].astype(bf16)
    fy_ref[...] = jnp.concatenate([cy, -sy], axis=0).astype(bf16)
    double = jnp.where(lax.broadcasted_iota(jnp.int32, (KY, 128), 0) == 0, 1.0, 2.0)
    iy_ref[...] = jnp.concatenate([double * cy, -(double * sy), blank], axis=0).T.astype(bf16)

    def step(i, carry):
        copy_in(u_hbm, u_buf, sems, i).wait()
        forward_group(i, u_buf, fy_ref[...], h_ref)
        return carry

    lax.fori_loop(0, steps, step, 0)
    modes_of(h_ref, m_ref, fx_ref, keep_ref, send_ref)


def layer_body(u_hbm, own_ref, oth_ref, ix_ref, iy_ref, w_ref, b_ref, out_hbm, u_buf, bs_ref, g_ref, sems, forward):
    steps = u_buf.shape[0] // GROUP
    for i in range(steps):
        copy_in(u_hbm, u_buf, sems.at[0], i).start()

    def unpack(k, carry):
        bs_ref[pl.ds(k * SC, RC), :] = own_ref[k].astype(jnp.float32)
        bs_ref[pl.ds((ZN + k) * SC, RC), :] = oth_ref[k].astype(jnp.float32)
        return carry

    lax.fori_loop(0, ZN, unpack, 0)
    scale = 1.0 / math.sqrt(2 * KX * KY)
    ix = ix_ref[...]
    for q in range(0, KY, 2):
        rhs = jnp.concatenate(
            [
                jnp.concatenate(
                    [bs_ref[pl.ds((q + d) * 4 + s, 16, stride=SC), :] for s in range(4)], axis=0
                ).astype(jnp.bfloat16)
                for d in range(2)
            ],
            axis=1,
        )
        for part in range(2):
            g = dot(ix[128 * part : 128 * part + 128], rhs) * scale
            for d in range(2):
                g_ref[pl.ds(part * KY + q + d, 128, stride=SG), :] = g[:, 128 * d : 128 * d + 128]

    def store(i):
        return pltpu.make_async_copy(
            u_buf.at[pl.ds(i * GROUP, GROUP)], out_hbm.at[pl.ds(i * GROUP, GROUP)], sems.at[1, i]
        )

    def point(i):
        w = w_ref[...]
        iy = iy_ref[...]
        bias = b_ref[...]
        pad = jnp.zeros((128 - 2 * KY, 128), jnp.bfloat16)
        for e in range(GROUP):
            x = i * GROUP + e
            gx = g_ref[pl.ds(x * SG, 2 * KY), :].astype(jnp.bfloat16)
            lhs = jnp.concatenate([u_buf[x], iy], axis=1)
            rhs = jnp.concatenate([w, gx, pad], axis=0)
            z = dot(lhs, rhs) + bias
            half = 0.5 * z
            u_buf[x] = (half + half * lax.erf(z * math.sqrt(0.5))).astype(jnp.bfloat16)

    def step(i, carry):
        copy_in(u_hbm, u_buf, sems.at[0], i).wait()
        if forward is not None:
            forward(i - 1)
        point(i)
        store(i).start()
        return carry

    copy_in(u_hbm, u_buf, sems.at[0], 0).wait()
    point(0)
    store(0).start()
    lax.fori_loop(1, steps, step, 0)
    if forward is not None:
        forward(steps - 1)

    def finish():
        for i in range(steps):
            store(i).wait()

    return finish


def mid_kernel(
    u_hbm, own_ref, oth_ref, ix_ref, iy_ref, w_ref, b_ref, fy_ref, fx_ref,
    out_hbm, keep_ref, send_ref, u_buf, bs_ref, g_ref, h_ref, m_ref, sems,
):
    def forward(i):
        forward_group(i, u_buf, fy_ref[...], h_ref)

    finish = layer_body(
        u_hbm, own_ref, oth_ref, ix_ref, iy_ref, w_ref, b_ref, out_hbm, u_buf, bs_ref, g_ref, sems, forward
    )
    modes_of(h_ref, m_ref, fx_ref, keep_ref, send_ref)
    finish()


def last_kernel(
    u_hbm, own_ref, oth_ref, ix_ref, iy_ref, w_ref, b_ref, out_hbm, u_buf, bs_ref, g_ref, sems
):
    layer_body(
        u_hbm, own_ref, oth_ref, ix_ref, iy_ref, w_ref, b_ref, out_hbm, u_buf, bs_ref, g_ref, sems, None
    )()


def split_kernel(spectral_hbm, first_ref, *refs):
    outs, buf, sems = refs[:-2], refs[-2], refs[-1]
    first = pltpu.make_async_copy(spectral_hbm.at[0], first_ref, sems.at[0, 0])
    loads = [pltpu.make_async_copy(spectral_hbm.at[n + 1], buf.at[n], sems.at[0, n + 1]) for n in range(len(outs))]
    stores = [pltpu.make_async_copy(buf.at[n], out, sems.at[1, n + 1]) for n, out in enumerate(outs)]
    for c in loads:
        c.start()
    first.start()
    for load, store in zip(loads, stores):
        load.wait()
        store.start()
    first.wait()
    for c in stores:
        c.wait()


def turn_kernel(s_ref, *refs):
    outs, t_ref = refs[:-1], refs[-1]
    a = s_ref[0].astype(jnp.float32)
    for k in range(1, ZN):
        a = a + s_ref[k].astype(jnp.float32)
    t_ref[...] = a.T
    y = lax.axis_index("mem") // SIDE
    for k in range(SIDE):
        start = pl.multiple_of((y + k) % SIDE * SLICE, SLICE)
        outs[k][...] = t_ref[pl.ds(start, SLICE), :].astype(jnp.bfloat16)


def share_kernel(*refs):
    a_refs, w_refs, outs = refs[:SIDE], refs[SIDE : 2 * SIDE], refs[2 * SIDE : 3 * SIDE]
    t_ref, m_ref, w_buf, sems = refs[3 * SIDE :]
    x = lax.axis_index("mem") % SIDE
    loads = [
        pltpu.make_async_copy(w_refs[k], w_buf.at[(x + SIDE - k) % SIDE], sems.at[k]) for k in range(SIDE)
    ]
    for c in loads:
        c.start()
    t_ref[...] = jnp.concatenate([r[...].astype(jnp.float32) for r in a_refs], axis=0).T
    row = lax.broadcasted_iota(jnp.int32, (8, 128), 0)
    lane = lax.broadcasted_iota(jnp.int32, (8, 128), 1)
    own = lane // SLICE == row
    for c in loads:
        c.wait()
    for q in range(KY):
        for jj in range(2):
            at = [q * 4 + 2 * ri + jj for ri in range(2)]
            lhs = jnp.concatenate(
                [jnp.where(own, t_ref[r : r + 1, :], 0.0) for r in at], axis=0
            ).astype(jnp.bfloat16)
            w = jnp.concatenate(
                [
                    jnp.concatenate([w_buf[x, jj, ri, q].astype(jnp.float32) for x in range(SIDE)] * SIDE, axis=0)
                    for ri in range(2)
                ],
                axis=1,
            ).astype(jnp.bfloat16)
            out = dot(lhs, w)
            re, im = out[:8], out[8:]
            m_ref[pl.ds(at[0], 8, stride=SC), :] = re[:, :128] - im[:, 128:]
            m_ref[pl.ds(at[1], 8, stride=SC), :] = re[:, 128:] + im[:, :128]
    for k in range(SIDE):
        outs[k][...] = m_ref[pl.ds(k * SC, RC), :].astype(jnp.bfloat16)


def total_kernel(*refs):
    out_ref = refs[-1]
    b = refs[0][...].astype(jnp.float32)
    for r in refs[1:-1]:
        b = b + r[...].astype(jnp.float32)
    b = b.astype(jnp.bfloat16)
    for k in range(ZN):
        out_ref[k] = b


def many_kernel(a_ref, w_hbm, out_ref, w_buf, sems):
    loads = [
        pltpu.make_async_copy(w_hbm.at[:, :, :, pl.ds(4 * b, 4)], w_buf.at[b], sems.at[b])
        for b in range(KY // 4)
    ]
    for c in loads:
        c.start()
    row = lax.broadcasted_iota(jnp.int32, (16, 128), 0)
    lower = row % 4 < 2
    blocks = []
    for b in range(KY // 4):
        rows = a_ref[16 * b : 16 * b + 16]
        acc = None
        loads[b].wait()
        for dq in range(4):
            for jj in range(2):
                mine = (row == dq * 4 + jj) | (row == dq * 4 + 2 + jj)
                lhs = jnp.where(mine, rows, 0)
                w = jnp.concatenate(
                    [
                        w_buf[b, :, jj, ri, dq].astype(jnp.float32).reshape(128, 128).astype(jnp.bfloat16)
                        for ri in range(2)
                    ],
                    axis=1,
                )
                part = dot(lhs, w)
                acc = part if acc is None else acc + part
        straight = acc[:, :128]
        cross = acc[:, 128:]
        up = jnp.concatenate([cross[2:], cross[:2]], axis=0)
        down = jnp.concatenate([cross[14:], cross[:14]], axis=0)
        blocks.append(jnp.where(lower, straight - up, straight + down).astype(jnp.bfloat16))
    full = jnp.concatenate(blocks, axis=0)
    for k in range(ZN):
        out_ref[k] = full


V = pl.BlockSpec(memory_space=pltpu.VMEM)
H = pl.BlockSpec(memory_space=pltpu.HBM)
A = pl.BlockSpec(memory_space=pl.ANY)


def call(kernel, args, outs, scratch=(), in_hbm=(), out_hbm=(), anywhere=(), limit=24):
    args = [
        pltpu.with_memory_space_constraint(a, pltpu.HBM) if i in in_hbm else a for i, a in enumerate(args)
    ]
    outs = [pltpu.HBM(o.shape, o.dtype) if i in out_hbm else o for i, o in enumerate(outs)]
    return pl.pallas_call(
        kernel,
        out_shape=outs,
        in_specs=[H if i in in_hbm else A if i in anywhere else V for i in range(len(args))],
        out_specs=[H if i in out_hbm else V for i in range(len(outs))],
        scratch_shapes=list(scratch),
        compiler_params=pltpu.CompilerParams(vmem_limit_bytes=limit << 20),
    )(*args)


def local(field, spectral, pointwise, bias):
    u = field[0]
    rows_here, cols_here, channels = u.shape
    bf16, f32 = jnp.bfloat16, jnp.float32
    sds = jax.ShapeDtypeStruct
    dma = pltpu.SemaphoreType.DMA
    chunks = [sds((ZN, RC, channels), f32), sds((ZN, RC, channels), bf16)]
    ub = pltpu.VMEM(u.shape, bf16)
    bs = pltpu.VMEM((2 * ZN * SC, channels), f32)
    gs = pltpu.VMEM((rows_here * SG, channels), f32)
    hs = pltpu.VMEM((2 * KY * SC, channels), f32)
    steps = rows_here // GROUP

    level_weights = sds(spectral.shape[1:], bf16)
    split = call(
        split_kernel, (spectral,), [level_weights] * LAYERS,
        (pltpu.VMEM((LAYERS - 1, *spectral.shape[1:]), bf16), dma((2, LAYERS))),
        in_hbm=(0,), out_hbm=tuple(range(1, LAYERS)),
    )
    weights = {}

    def gather(level, block):
        weights[level] = lax.all_gather(block, "mem")

    gather(1, split[1])
    near = [split[0]]
    for k in range(1, SIDE):
        near.append(lax.ppermute(split[0], "mem", shift(0, k)))

    cosines, sines = angle_tables(rows_here, cols_here)
    keep, send, forward_x, inverse_x, forward_y, inverse_y = call(
        first_kernel,
        (u, cosines, sines),
        [
            *chunks,
            sds((2 * KX, 2 * rows_here), bf16),
            sds((2 * rows_here, 2 * KX), bf16),
            sds((2 * KY, cols_here), bf16),
            sds((cols_here, 128), bf16),
        ],
        (ub, hs, bs, dma((steps,))),
        in_hbm=(0,),
    )
    for level in range(LAYERS):
        other = lax.ppermute(send, GRID, PAIR)
        paired = (keep + other.astype(f32)).astype(bf16)
        parts = lax.all_to_all(paired, GRID, 0, 0, axis_index_groups=LINES, tiled=True)
        if level == 0:
            square = pltpu.VMEM((RC, channels), f32)
            slices = call(turn_kernel, (parts,), [sds((SLICE, RC), bf16)] * SIDE, (square,))
            slices = [slices[0]] + [lax.ppermute(slices[k], "mem", shift(k, 0)) for k in range(1, SIDE)]
            shares = call(
                share_kernel,
                (*slices, *near),
                [sds((RC, channels), bf16)] * SIDE,
                (
                    square,
                    pltpu.VMEM((8 * SC, channels), f32),
                    pltpu.VMEM((SIDE, *spectral.shape[1:]), bf16),
                    dma((SIDE,)),
                ),
                anywhere=tuple(range(SIDE, 2 * SIDE)),
            )
            shares = [shares[0]] + [lax.ppermute(shares[k], "mem", shift(-k, 0)) for k in range(1, SIDE)]
            (mixed,) = call(total_kernel, shares, [sds((ZN, RC, channels), bf16)])
        else:
            coeffs = parts.astype(f32).sum(axis=0).astype(bf16)
            (mixed,) = call(
                many_kernel,
                (coeffs, weights[level]),
                [sds((ZN, RC, channels), bf16)],
                (
                    pltpu.VMEM((KY // 4, lax.axis_size("mem"), 2, 2, 4, 8, channels), bf16),
                    dma((KY // 4,)),
                ),
                in_hbm=(1,),
            )
        own = lax.all_to_all(mixed, GRID, 0, 0, axis_index_groups=LINES, tiled=True)
        if level < LAYERS - 2:
            own, block = lax.optimization_barrier((own, split[level + 2]))
            gather(level + 2, block)
        oth = lax.ppermute(own, GRID, PAIR)
        args = (u, own, oth, inverse_x, inverse_y, pointwise[level], bias[level][None])
        if level < LAYERS - 1:
            u, keep, send = call(
                mid_kernel,
                (*args, forward_y, forward_x),
                [sds(u.shape, bf16), *chunks],
                (ub, bs, gs, hs, bs, dma((2, steps))),
                in_hbm=(0,),
                out_hbm=(0,),
            )
        else:
            (u,) = call(
                last_kernel, args, [sds(u.shape, bf16)], (ub, bs, gs, dma((2, steps))),
                in_hbm=(0,), out_hbm=(0,),
            )
    return u[None]


def solution(mesh):
    in_specs = (
        P("mem", "gx", "gy", None),
        P(None, ("gx", "gy"), None, None, "mem", None),
        P(),
        P(),
    )
    out_specs = P("mem", "gx", "gy", None)
    return jax.shard_map(local, mesh=mesh, in_specs=in_specs, out_specs=out_specs, check_vma=False)
```
